32 devices in a mesh: groups: 2 (over y), gx: 4 (over z), gy: 2 (over x), gz: 2 (over core).
Axes of the slice: x: 2, y: 2, z: 4, core: 2. Of those that a mesh axis runs over, the one named last changes fastest.
Arguments:
- latents: bfloat16 [8, 2, 2, 128, 128], P(('groups', 'gx'), 'gy', 'gz'), parts along dimension 0, may hold values from -6 to 6
- offsets: bfloat16 [8, 2, 2, 3, 128], P(('groups', 'gx'), 'gy', 'gz'), parts along dimension 0, may hold values from 0 to 1
- neighbours: int32 [8, 2, 2, 384], P(('groups', 'gx'), 'gy', 'gz'), parts along dimension 0, may hold values from 0 to 2047, as said below
- counts: int32 [8, 2, 2], P(('groups', 'gx'), 'gy', 'gz'), parts along dimension 0, may hold values from 1 to 384, as said below
- w_recv: bfloat16 [1, 128, 128], replicated, may hold values from -0.5 to 0.5
- w_send: bfloat16 [1, 128, 128], replicated, may hold values from -0.5 to 0.5
- w_rel: bfloat16 [1, 4, 128], replicated, may hold values from -3 to 3
- b_first: float32 [1, 128], replicated, may hold values from -5 to 5
- w_edge: bfloat16 [1, 128, 128], replicated, may hold values from -0.5 to 0.5
- b_edge: float32 [1, 128], replicated, may hold values from -5 to 5
- w_self: bfloat16 [1, 128, 128], replicated, may hold values from -0.5 to 0.5
- w_agg: bfloat16 [1, 128, 128], replicated, may hold values from -0.5 to 0.5
- w_out: bfloat16 [1, 128, 128], replicated, may hold values from -0.5 to 0.5
- norm_gain: float32 [1, 128], replicated, may hold values from 0.1 to 1.9
Outputs:
- processed: bfloat16 [8, 2, 2, 128, 128], P(('groups', 'gx'), 'gy', 'gz'), parts along dimension 0
The draws below stay inside these ranges and needn't reach their ends.
There are 2 independent parts, one for each index of `groups`. The reference program is written for one: setup_inputs(seed, part) draws one part's arguments, and reference() takes and returns one part's arrays. A program takes and returns all parts, laid end to end along the dimension named above; an argument that names none is the same for every part. Nothing has to cross between parts.
Inputs may be any that keep to these rules, and one draw needn't show every extreme that they name: `neighbours`: each sender is a particle of the same cell or of a cell whose three coordinates differ from the receiver cell's by at most one. Only the first counts[cell] senders of a cell are live, the rest is padding. In the cells whose first coordinate is below 1 all 384 senders are live.
All inputs are finite; a program needn't handle non-finite values.
Results may differ from the reference program's by a relative error of at most 0.0055.
Values may be sent and summed in bfloat16 or wider, within the bound.
A program may use at most 64 MiB of HBM per device.

```python
import jax
import jax.numpy as jnp
from jax import lax

W = 128
SLOTS = 128
NBLK = 3
STEPS = 1
NX = 4
NY = 2
NZ = 2


def draw_neighbours(key, part):
    draw_shape = (NX, NY, NZ, NBLK * SLOTS)
    subkeys = jax.random.split(jax.random.fold_in(key, 11), 4)
    axis_x = jnp.arange(NX, dtype=jnp.int32)[:, None, None, None]
    axis_y = jnp.arange(NY, dtype=jnp.int32)[None, :, None, None]
    axis_z = jnp.arange(NZ, dtype=jnp.int32)[None, None, :, None]
    coord_x = jnp.clip(axis_x + jax.random.randint(subkeys[0], draw_shape, -1, 2), 0, NX - 1)
    coord_y = jnp.clip(axis_y + jax.random.randint(subkeys[1], draw_shape, -1, 2), 0, NY - 1)
    coord_z = jnp.clip(axis_z + jax.random.randint(subkeys[2], draw_shape, -1, 2), 0, NZ - 1)
    slot_pick = jax.random.randint(subkeys[3], draw_shape, 0, SLOTS)
    return (((coord_x * NY + coord_y) * NZ + coord_z) * SLOTS + slot_pick).astype(jnp.int32)


def draw_counts(key, part):
    axis_x = jnp.arange(NX, dtype=jnp.int32)[:, None, None]
    sparse = jax.random.randint(jax.random.fold_in(key, 23), (NX, NY, NZ), 1, SLOTS + 1)
    packed = jnp.full((NX, NY, NZ), NBLK * SLOTS, jnp.int32)
    return jnp.where(axis_x < NX // 4, packed, sparse).astype(jnp.int32)


def levels(key, extent, pieces, smallest, largest):
    loudness, own = 1.0, jax.random.fold_in(key, 6)
    for axis_at, shards_of in pieces:
        draws = jnp.exp(jax.random.uniform(jax.random.fold_in(own, axis_at), (shards_of,), jnp.float32, smallest / len(pieces), largest / len(pieces)))
        loudness = loudness * jnp.repeat(draws, extent[axis_at] // shards_of).reshape([-1 if axis == axis_at else 1 for axis in range(len(extent))])
    return loudness


def scatter_about(own_key, dims, width, limit, shards=(), kind=jnp.bfloat16):
    factor_of = levels(own_key, dims, shards, -0.22, 0.18) if shards else 1.0
    values = jax.random.normal(own_key, dims, jnp.float32) * width * factor_of
    return jnp.minimum(jnp.maximum(values, -limit), limit).astype(kind)


def setup_inputs(seed: int = 0, part: int = 0) -> dict:
    arg_keys = jax.random.split(jax.random.key(seed), 15)
    own_keys = jax.random.split(jax.random.fold_in(arg_keys[14], part), 15)
    latents = scatter_about(own_keys[0], (NX, NY, NZ, SLOTS, W), 1.0, 6.0, ((0, 4), (1, 2), (2, 2)))
    offsets = jnp.clip(1.0 * jax.random.uniform(own_keys[1], (NX, NY, NZ, 3, SLOTS), jnp.float32) ** levels(own_keys[1], (NX, NY, NZ, 3, SLOTS), ((0, 4), (1, 2), (2, 2)), -0.2, 0.2), 0.0, 1.0).astype(jnp.bfloat16)
    neighbours = draw_neighbours(jax.random.fold_in(jax.random.fold_in(arg_keys[14], part), 71), part)
    counts = draw_counts(jax.random.fold_in(jax.random.fold_in(arg_keys[14], part), 71), part)
    w_recv = scatter_about(arg_keys[4], (STEPS, W, W), W ** -0.5, 0.5)
    w_send = scatter_about(arg_keys[5], (STEPS, W, W), W ** -0.5, 0.5)
    w_rel = scatter_about(arg_keys[6], (STEPS, 4, W), 4 ** -0.5, 3.0)
    b_first = scatter_about(arg_keys[7], (STEPS, W), 1.0, 5.0, (), jnp.float32)
    w_edge = scatter_about(arg_keys[8], (STEPS, W, W), W ** -0.5, 0.5)
    b_edge = scatter_about(arg_keys[9], (STEPS, W), 1.0, 5.0, (), jnp.float32)
    w_self = scatter_about(arg_keys[10], (STEPS, W, W), W ** -0.5, 0.5)
    w_agg = scatter_about(arg_keys[11], (STEPS, W, W), W ** -0.5, 0.5)
    w_out = scatter_about(arg_keys[12], (STEPS, W, W), W ** -0.5, 0.5)
    norm_gain = jnp.clip(1.0 + 0.18 * jax.random.normal(arg_keys[13], (STEPS, W), jnp.float32), 0.1, 1.9)
    return {"latents": latents, "offsets": offsets, "neighbours": neighbours, "counts": counts, "w_recv": w_recv, "w_send": w_send, "w_rel": w_rel, "b_first": b_first, "w_edge": w_edge, "b_edge": b_edge, "w_self": w_self, "w_agg": w_agg, "w_out": w_out, "norm_gain": norm_gain}


def edge_sum(recv_term, send_term, recv_place, send_place, live_mask, rel_weight, w_edge, b_edge):
    row_count, latent_width = recv_term.shape
    tile_rows = min(16, row_count)
    tile_count = row_count // tile_rows

    def tile_messages(operands):
        recv_tile, place_tile = operands
        relative = send_place[:, None, :] - place_tile[:, :, None]
        features = jnp.concatenate([relative, 0.25 * lax.optimization_barrier(jnp.sum(relative * relative, axis=0, keepdims=True))], axis=0)
        place_term = jnp.einsum('cij,cw->ijw', features, rel_weight, precision=lax.Precision.HIGHEST)
        pre_act = recv_tile[:, None, :] + send_term[None, :, :] + place_term
        edge_act = jax.nn.silu(pre_act).astype(jnp.bfloat16)
        message = jnp.dot(edge_act.reshape(-1, latent_width), w_edge, preferred_element_type=jnp.float32) + b_edge
        message = jax.nn.silu(message).reshape(tile_rows, -1, latent_width)
        return jnp.einsum('ijw,j->iw', message, live_mask, precision=lax.Precision.HIGHEST)
    recv_tiles = recv_term.reshape(tile_count, tile_rows, latent_width)
    place_tiles = recv_place.reshape(3, tile_count, tile_rows).transpose(1, 0, 2)
    return lax.map(tile_messages, (recv_tiles, place_tiles)).reshape(row_count, latent_width)

def renew(latent, summed, w_self, w_agg, w_out, norm_gain):
    pooled = (summed / latent.shape[0]).astype(jnp.bfloat16)
    hidden = jax.nn.silu(jnp.dot(latent, w_self, preferred_element_type=jnp.float32) + jnp.dot(pooled, w_agg, preferred_element_type=jnp.float32)).astype(jnp.bfloat16)
    result = jnp.dot(hidden, w_out, preferred_element_type=jnp.float32)
    center = lax.optimization_barrier(jnp.mean(result, axis=-1, keepdims=True))
    spread = lax.optimization_barrier(jnp.mean((result - center) ** 2, axis=-1, keepdims=True))
    normed = (result - center) * lax.rsqrt(spread + 1e-05) * norm_gain
    return (latent.astype(jnp.float32) + normed).astype(jnp.bfloat16)

def reference(latents, offsets, neighbours, counts, w_recv, w_send, w_rel, b_first, w_edge, b_edge, w_self, w_agg, w_out, norm_gain):
    cell_count = NX * NY * NZ
    current = latents.reshape(cell_count, SLOTS, W)
    cell_ids = jnp.arange(cell_count, dtype=jnp.int32)
    coords = jnp.stack([cell_ids // (NY * NZ), cell_ids // NZ % NY, cell_ids % NZ], axis=1).astype(jnp.float32)
    places = offsets.reshape(cell_count, 3, SLOTS).astype(jnp.float32) + coords[:, :, None]
    flat_places = places.transpose(1, 0, 2).reshape(3, cell_count * SLOTS)
    neighbour_rows = neighbours.reshape(cell_count, NBLK * SLOTS)
    count_rows = counts.reshape(cell_count)
    slot_ids = jnp.arange(SLOTS, dtype=jnp.int32)
    for step_index in range(STEPS):
        flat_latents = current.reshape(cell_count * SLOTS, W)
        rel_weight = w_rel[step_index].astype(jnp.float32)

        def update_cell(operands, step_index=step_index, flat_latents=flat_latents, rel_weight=rel_weight):
            latent, recv_place, sender_row, sender_count = operands
            recv_term = jnp.dot(latent, w_recv[step_index], preferred_element_type=jnp.float32) + b_first[step_index]
            summed = jnp.zeros((SLOTS, W), jnp.float32)
            for block_index in range(NBLK):
                sender_ids = sender_row[block_index * SLOTS:(block_index + 1) * SLOTS]
                gathered = jnp.take(flat_latents, sender_ids, axis=0)
                send_term = jnp.dot(gathered, w_send[step_index], preferred_element_type=jnp.float32)
                send_place = jnp.take(flat_places, sender_ids, axis=1)
                live_mask = (block_index * SLOTS + slot_ids < sender_count).astype(jnp.float32)
                summed = summed + edge_sum(recv_term, send_term, recv_place, send_place, live_mask, rel_weight, w_edge[step_index], b_edge[step_index])
            return renew(latent, summed, w_self[step_index], w_agg[step_index], w_out[step_index], norm_gain[step_index])
        current = lax.map(update_cell, (current, places, neighbour_rows, count_rows))
    return current.reshape(NX, NY, NZ, SLOTS, W)
```

```python
import functools

import jax
import jax.numpy as jnp
from jax import lax
from jax.experimental import pallas as pl
from jax.experimental.pallas import tpu as pltpu
from jax.sharding import PartitionSpec as P

MESH = pl.DeviceIdType.MESH
PACK = 16
GROUP = 16


def split(value, size):
    if size & (size - 1) == 0:
        return value >> (size.bit_length() - 1), value & (size - 1)
    return lax.div(value, size), lax.rem(value, size)


def wide(axis):
    return lax.axis_size(axis) > 2


def slots_of(axis):
    return min(lax.axis_size(axis), 3)


def moves(axis):
    size, here = lax.axis_size(axis), lax.axis_index(axis)
    if size == 1:
        return []
    if size == 2:
        return [(1 - here, None)]
    return [(here - 1, here > 0), (here + 1, here < size - 1)]


def slot_on(axis, source, target):
    return source - target + 1 if wide(axis) else source


def both(a, b):
    if a is None:
        return b
    return a if b is None else jnp.logical_and(a, b)


def guarded(condition, action):
    if condition is None:
        action()
    else:
        pl.when(condition)(action)


def kernel(
    counts_ref, latents_ref, offsets_ref, neighbours_ref, w_recv, w_send, w_rel, b_first, w_edge,
    b_edge, w_self, w_agg, w_out, norm_gain, out_ref, table, recv_half, send_half, scaled, pooled,
    pair_edge, send_sem, recv_sem, relay_sem,
):
    f32, bf16 = jnp.float32, jnp.bfloat16
    slots, width = latents_ref.shape[3], latents_ref.shape[4]
    senders = neighbours_ref.shape[3]
    blocks = senders // slots
    here = [lax.axis_index(axis) for axis in ("gx", "gy", "gz")]
    sizes = [lax.axis_size(axis) for axis in ("gx", "gy", "gz")]
    spans = [slots_of(axis) for axis in ("gx", "gy", "gz")]

    def slot(coords):
        return (coords[0] * spans[1] + coords[1]) * spans[2] + coords[2]

    own_coords = [slot_on(a, c, c) for a, c in zip(("gx", "gy", "gz"), here)]
    own = slot(own_coords)

    latent = latents_ref[0, 0, 0]
    place = offsets_ref[0, 0, 0].astype(f32)
    rows = lax.broadcasted_iota(jnp.int32, (PACK, slots), 0)
    extra = jnp.zeros((PACK, slots), f32)
    for c in range(3):
        extra = jnp.where(rows == c, place[c : c + 1, :], extra)
        extra = jnp.where(rows == 3 + c, here[c].astype(f32), extra)
    table[own, :slots, :] = latent
    table[own, slots:, :] = extra.astype(bf16)

    stay_x, stay_y = (here[0], None), (here[1], None)
    routes = []
    for x, when_x in [stay_x] + moves("gx"):
        for y, when_y in [stay_y] + moves("gy"):
            if x is here[0] and y is here[1]:
                continue
            routes.append((x, y, both(when_x, when_y)))
    routes.sort(key=lambda r: (r[0] is not here[0]) + (r[1] is not here[1]))
    has_mate = sizes[2] > 1
    mate = {"gz": 1 - here[2]}

    barrier = pltpu.get_barrier_semaphore()

    def hello(target):
        pl.semaphore_signal(barrier, inc=1, device_id=target, device_id_type=MESH)

    if has_mate:
        hello(mate)
    for x, y, when in routes:
        guarded(when, functools.partial(hello, {"gx": x, "gy": y}))
    peers = jnp.int32(1 if has_mate else 0)
    for x, y, when in routes:
        peers = peers + (1 if when is None else when.astype(jnp.int32))
    pl.semaphore_wait(barrier, peers)

    sends, relays = [], []
    for n, (x, y, when) in enumerate(routes):
        there = slot(
            [slot_on("gx", here[0], x), slot_on("gy", here[1], y), slot_on("gz", here[2], here[2])]
        )
        mine = slot(
            [slot_on("gx", x, here[0]), slot_on("gy", y, here[1]), slot_on("gz", here[2], here[2])]
        )
        copy = pltpu.make_async_remote_copy(
            src_ref=table.at[own],
            dst_ref=table.at[there],
            send_sem=send_sem.at[n],
            recv_sem=recv_sem.at[there],
            device_id={"gx": x, "gy": y},
            device_id_type=MESH,
        )
        arrival = pltpu.make_async_remote_copy(
            src_ref=table.at[own],
            dst_ref=table.at[mine],
            send_sem=send_sem.at[n],
            recv_sem=recv_sem.at[mine],
            device_id={"gx": x, "gy": y},
            device_id_type=MESH,
        )
        relay = pltpu.make_async_remote_copy(
            src_ref=table.at[mine],
            dst_ref=table.at[mine],
            send_sem=relay_sem.at[n],
            recv_sem=recv_sem.at[mine],
            device_id=mate,
            device_id_type=MESH,
        )
        mate_slot = slot(
            [slot_on("gx", x, here[0]), slot_on("gy", y, here[1]), 1 - here[2]]
        )
        mate_arrival = pltpu.make_async_remote_copy(
            src_ref=table.at[own],
            dst_ref=table.at[mate_slot],
            send_sem=relay_sem.at[n],
            recv_sem=recv_sem.at[mate_slot],
            device_id=mate,
            device_id_type=MESH,
        )
        sends.append((when, copy, arrival, mine))
        relays.append((relay, mate_arrival, mate_slot))
    last = len(routes)
    if has_mate:
        mate_own = slot([own_coords[0], own_coords[1], 1 - here[2]])
        mate_copy = pltpu.make_async_remote_copy(
            src_ref=table.at[own], dst_ref=table.at[own], send_sem=send_sem.at[last],
            recv_sem=recv_sem.at[own], device_id=mate, device_id_type=MESH,
        )
        mate_in = pltpu.make_async_remote_copy(
            src_ref=table.at[own], dst_ref=table.at[mate_own], send_sem=send_sem.at[last],
            recv_sem=recv_sem.at[mate_own], device_id=mate, device_id_type=MESH,
        )
    for when, copy, _, _ in sends:
        guarded(when, copy.start)
    if has_mate:
        mate_copy.start()

    def clear(which):
        table[which] = jnp.zeros(table.shape[1:], bf16)

    for (when, _, _, mine), (_, _, mate_slot) in zip(sends, relays):
        if when is not None:
            pl.when(jnp.logical_not(when))(functools.partial(clear, mine))
            if has_mate:
                pl.when(jnp.logical_not(when))(functools.partial(clear, mate_slot))

    cell, at = split(neighbours_ref[0, 0], slots)
    cell, z = split(cell, sizes[2])
    x, y = split(cell, sizes[1])
    found = [
        v - h + 1 if wide(a) else v for a, v, h in zip(("gx", "gy", "gz"), (x, y, z), here)
    ]
    row_ids = (slot(found) * slots + at).astype(f32)
    ids = jnp.concatenate(
        [
            jnp.broadcast_to(row_ids[:, b * slots : (b + 1) * slots], (slots, slots)).T
            for b in range(blocks)
        ],
        axis=0,
    ).astype(jnp.int32)
    lanes = lax.broadcasted_iota(jnp.int32, (senders, slots), 1)
    count = table.shape[0]
    chosen = jnp.concatenate(
        [jnp.where(ids - k * slots == lanes, 1.0, 0.0).astype(bf16) for k in range(count)], axis=1
    )

    rel = w_rel[0].astype(f32)
    place_cols = jnp.transpose(jnp.broadcast_to(place[:1], (slots, slots)))
    recv = jnp.dot(latent, w_recv[0], preferred_element_type=f32) + b_first[...]
    for c in range(3):
        if c:
            place_cols = jnp.transpose(jnp.broadcast_to(place[c : c + 1], (slots, slots)))
        recv = recv - place_cols * rel[c : c + 1]
    recv_half[...] = 0.5 * recv

    for (when, _, arrival, _), (relay, _, _) in zip(sends, relays):

        def pass_on(arrival=arrival, relay=relay):
            arrival.wait_recv()
            if has_mate:
                relay.start()

        guarded(when, pass_on)
    if has_mate:
        mate_in.wait_recv()
        for (when, _, _, _), (_, mate_arrival, _) in zip(sends, relays):
            guarded(when, mate_arrival.wait_recv)

    gathered = jnp.dot(
        chosen, table[:, :slots, :].reshape(count * slots, width), preferred_element_type=f32
    ).astype(bf16)
    feats = jnp.zeros((senders, PACK), f32)
    for k in range(count):
        feats = feats + lax.dot_general(
            chosen[:, k * slots : (k + 1) * slots],
            table[k, slots:, :],
            (((1,), (1,)), ((), ())),
            preferred_element_type=f32,
        )
    send = jnp.dot(gathered, w_send[0], preferred_element_type=f32)
    square = jnp.zeros((senders, slots), f32)
    for c in range(3):
        where = feats[:, c : c + 1] + (feats[:, 3 + c : 4 + c] - here[c].astype(f32))
        where = jnp.broadcast_to(where, (senders, slots))
        send = send + where * rel[c : c + 1]
        apart = where - place[c : c + 1]
        square = square + apart * apart
    send_half[...] = (0.5 * send).astype(bf16)
    scaled[...] = 0.25 * square

    rel_half = (0.5 * rel[3:4]).astype(bf16)
    edge_half = 0.5 * w_edge[0].astype(f32)
    nil = jnp.zeros_like(edge_half)
    pair_edge[...] = jnp.concatenate(
        [jnp.concatenate([edge_half, nil], axis=1), jnp.concatenate([nil, edge_half], axis=1)], axis=0
    ).astype(bf16)
    bias_half = (0.5 * b_edge[...]).astype(bf16)
    bias_pair = jnp.concatenate([bias_half, bias_half], axis=1)
    live = (
        lax.broadcasted_iota(jnp.int32, (8, senders), 1) < counts_ref[0]
    ).astype(f32).astype(bf16)

    @pl.loop(0, slots // GROUP)
    def _(group):
        base = pl.multiple_of(group * GROUP, GROUP)
        own_rows = recv_half[pl.ds(base, GROUP), :].astype(bf16)
        sums = []
        for i in range(0, GROUP, 2):
            total = jnp.zeros((8, 2 * width), f32)
            for b in range(blocks):
                span = slice(b * slots, (b + 1) * slots)
                halves = []
                for n in (i, i + 1):
                    s = jnp.broadcast_to(scaled[span, n : n + 1], (slots, width)).astype(bf16)
                    pre = own_rows[n : n + 1] + send_half[span, :] + s * rel_half
                    halves.append(pre * (jnp.tanh(pre) + 1))
                edge = jnp.concatenate(halves, axis=1)
                msg = jnp.dot(edge, pair_edge[...], preferred_element_type=f32).astype(bf16)
                msg = msg + bias_pair
                msg = msg * (jnp.tanh(msg) + 1)
                total = total + jnp.dot(live[:, span], msg, preferred_element_type=f32)
            sums += [total[:1, :width], total[:1, width:]]
        pooled[pl.ds(base, GROUP), :] = jnp.concatenate(sums, axis=0)
        scaled[...] = pltpu.roll(scaled[...], slots - GROUP, 1)

    mean = (pooled[...] / slots).astype(bf16)
    hidden = jax.nn.silu(
        jnp.dot(latent, w_self[0], preferred_element_type=f32)
        + jnp.dot(mean, w_agg[0], preferred_element_type=f32)
    ).astype(bf16)
    result = jnp.dot(hidden, w_out[0], preferred_element_type=f32)
    center = jnp.mean(result, axis=-1, keepdims=True)
    shifted = result - center
    spread = jnp.mean(shifted * shifted, axis=-1, keepdims=True)
    normed = shifted * lax.rsqrt(spread + 1e-05) * norm_gain[...]
    out_ref[0, 0, 0] = (latent.astype(f32) + normed).astype(bf16)

    for (when, copy, _, _), (relay, _, _) in zip(sends, relays):

        def finish(copy=copy, relay=relay):
            copy.wait_send()
            if has_mate:
                relay.wait_send()

        guarded(when, finish)
    if has_mate:
        mate_copy.wait_send()


def shards(latents, offsets, neighbours, counts, *weights):
    slots, width = latents.shape[3:]
    senders = neighbours.shape[3]
    count = slots_of("gx") * slots_of("gy") * slots_of("gz")
    routes = 9
    f32, bf16 = jnp.float32, jnp.bfloat16
    vmem = pl.BlockSpec(memory_space=pltpu.VMEM)
    return pl.pallas_call(
        kernel,
        out_shape=jax.ShapeDtypeStruct(latents.shape, latents.dtype),
        in_specs=[vmem] * (4 + len(weights)),
        out_specs=vmem,
        scratch_shapes=[
            pltpu.VMEM((count, slots + PACK, width), bf16),
            pltpu.VMEM((slots, width), f32),
            pltpu.VMEM((senders, width), bf16),
            pltpu.VMEM((senders, slots), f32),
            pltpu.VMEM((slots, width), f32),
            pltpu.VMEM((2 * width, 2 * width), bf16),
            pltpu.SemaphoreType.DMA((routes,)),
            pltpu.SemaphoreType.DMA((count,)),
            pltpu.SemaphoreType.DMA((routes,)),
        ],
        compiler_params=pltpu.CompilerParams(collective_id=0, has_side_effects=True),
    )(counts, latents, offsets, neighbours, *weights)


def solution(mesh):
    cells = ("groups", "gx"), "gy", "gz"
    in_specs = (P(*cells, None, None), P(*cells, None, None), P(*cells, None), P(*cells))
    in_specs += (P(),) * 10
    return jax.shard_map(
        shards, mesh=mesh, in_specs=in_specs, out_specs=P(*cells, None, None), check_vma=False
    )
```

```python
import functools

import jax
import jax.numpy as jnp
from jax import lax
from jax.experimental import pallas as pl
from jax.experimental.pallas import tpu as pltpu
from jax.sharding import PartitionSpec as P

MESH = pl.DeviceIdType.MESH
PACK = 16
GROUP = 16
PAIRS = 1
INPUTS = 14
LOAD_ORDER = (1, 2, 3, 0) + tuple(range(4, 14))


def split(value, size):
    if size & (size - 1) == 0:
        return value >> (size.bit_length() - 1), value & (size - 1)
    return lax.div(value, size), lax.rem(value, size)


def wide(axis):
    return lax.axis_size(axis) > 2


def slots_of(axis):
    return min(lax.axis_size(axis), 3)


def moves(axis):
    size, here = lax.axis_size(axis), lax.axis_index(axis)
    if size == 1:
        return []
    if size == 2:
        return [(1 - here, None)]
    return [(here - 1, here > 0), (here + 1, here < size - 1)]


def slot_on(axis, source, target):
    return source - target + 1 if wide(axis) else source


def both(a, b):
    if a is None:
        return b
    return a if b is None else jnp.logical_and(a, b)


def guarded(condition, action):
    if condition is None:
        action()
    else:
        pl.when(condition)(action)


def kernel(*refs):
    hbm, out_ref, held, scratch = refs[:INPUTS], refs[INPUTS], refs[INPUTS + 1 : 2 * INPUTS + 1], refs[2 * INPUTS + 1 :]
    load_sem, table, recv_half, send_half, scaled, pooled, pair_edge, masked = scratch[:8]
    send_sem, recv_sem, relay_sem = scratch[8:]
    (
        counts_ref, latents_ref, offsets_ref, neighbours_ref, w_recv, w_send, w_rel, b_first,
        w_edge, b_edge, w_self, w_agg, w_out, norm_gain,
    ) = held
    loads = [
        pltpu.make_async_copy(src, dst, load_sem.at[n]) for n, (src, dst) in enumerate(zip(hbm, held))
    ]
    for n in LOAD_ORDER:
        loads[n].start()
    f32, bf16 = jnp.float32, jnp.bfloat16
    slots, width = latents_ref.shape[3], latents_ref.shape[4]
    senders = neighbours_ref.shape[3]
    blocks = senders // slots
    here = [lax.axis_index(axis) for axis in ("gx", "gy", "gz")]
    sizes = [lax.axis_size(axis) for axis in ("gx", "gy", "gz")]
    spans = [slots_of(axis) for axis in ("gx", "gy", "gz")]

    def slot(coords):
        return (coords[0] * spans[1] + coords[1]) * spans[2] + coords[2]

    own_coords = [slot_on(a, c, c) for a, c in zip(("gx", "gy", "gz"), here)]
    own = slot(own_coords)

    stay_x, stay_y = (here[0], None), (here[1], None)
    routes = []
    for x, when_x in [stay_x] + moves("gx"):
        for y, when_y in [stay_y] + moves("gy"):
            if x is here[0] and y is here[1]:
                continue
            routes.append((x, y, both(when_x, when_y)))
    routes.sort(key=lambda r: (r[0] is not here[0]) + (r[1] is not here[1]))
    has_mate = sizes[2] > 1
    mate = {"gz": 1 - here[2]}

    barrier = pltpu.get_barrier_semaphore()

    def hello(target):
        pl.semaphore_signal(barrier, inc=1, device_id=target, device_id_type=MESH)

    if has_mate:
        hello(mate)
    for x, y, when in routes:
        guarded(when, functools.partial(hello, {"gx": x, "gy": y}))
    for n in (1, 2):
        loads[n].wait()
    latent = latents_ref[0, 0, 0]
    place = offsets_ref[0, 0, 0].astype(f32)
    rows = lax.broadcasted_iota(jnp.int32, (PACK, slots), 0)
    extra = jnp.zeros((PACK, slots), f32)
    for c in range(3):
        extra = jnp.where(rows == c, place[c : c + 1, :], extra)
        extra = jnp.where(rows == 3 + c, here[c].astype(f32), extra)
    table[own, :slots, :] = latent
    table[own, slots:, :] = extra.astype(bf16)

    peers = jnp.int32(1 if has_mate else 0)
    for x, y, when in routes:
        peers = peers + (1 if when is None else when.astype(jnp.int32))
    pl.semaphore_wait(barrier, peers)

    sends, relays = [], []
    for n, (x, y, when) in enumerate(routes):
        there = slot(
            [slot_on("gx", here[0], x), slot_on("gy", here[1], y), slot_on("gz", here[2], here[2])]
        )
        mine = slot(
            [slot_on("gx", x, here[0]), slot_on("gy", y, here[1]), slot_on("gz", here[2], here[2])]
        )
        copy = pltpu.make_async_remote_copy(
            src_ref=table.at[own],
            dst_ref=table.at[there],
            send_sem=send_sem.at[n],
            recv_sem=recv_sem.at[there],
            device_id={"gx": x, "gy": y},
            device_id_type=MESH,
        )
        arrival = pltpu.make_async_remote_copy(
            src_ref=table.at[own],
            dst_ref=table.at[mine],
            send_sem=send_sem.at[n],
            recv_sem=recv_sem.at[mine],
            device_id={"gx": x, "gy": y},
            device_id_type=MESH,
        )
        relay = pltpu.make_async_remote_copy(
            src_ref=table.at[mine],
            dst_ref=table.at[mine],
            send_sem=relay_sem.at[n],
            recv_sem=recv_sem.at[mine],
            device_id=mate,
            device_id_type=MESH,
        )
        mate_slot = slot(
            [slot_on("gx", x, here[0]), slot_on("gy", y, here[1]), 1 - here[2]]
        )
        mate_arrival = pltpu.make_async_remote_copy(
            src_ref=table.at[own],
            dst_ref=table.at[mate_slot],
            send_sem=relay_sem.at[n],
            recv_sem=recv_sem.at[mate_slot],
            device_id=mate,
            device_id_type=MESH,
        )
        sends.append((when, copy, arrival, mine))
        relays.append((relay, mate_arrival, mate_slot))
    last = len(routes)
    if has_mate:
        mate_own = slot([own_coords[0], own_coords[1], 1 - here[2]])
        mate_copy = pltpu.make_async_remote_copy(
            src_ref=table.at[own], dst_ref=table.at[own], send_sem=send_sem.at[last],
            recv_sem=recv_sem.at[own], device_id=mate, device_id_type=MESH,
        )
        mate_in = pltpu.make_async_remote_copy(
            src_ref=table.at[own], dst_ref=table.at[mate_own], send_sem=send_sem.at[last],
            recv_sem=recv_sem.at[mate_own], device_id=mate, device_id_type=MESH,
        )
    for when, copy, _, _ in sends:
        guarded(when, copy.start)
    if has_mate:
        mate_copy.start()

    def clear(which):
        table[which] = jnp.zeros(table.shape[1:], bf16)

    for (when, _, _, mine), (_, _, mate_slot) in zip(sends, relays):
        if when is not None:
            pl.when(jnp.logical_not(when))(functools.partial(clear, mine))
            if has_mate:
                pl.when(jnp.logical_not(when))(functools.partial(clear, mate_slot))

    loads[0].wait()
    for n in range(3, INPUTS):
        loads[n].wait()
    cell, at = split(neighbours_ref[0, 0], slots)
    cell, z = split(cell, sizes[2])
    x, y = split(cell, sizes[1])
    found = [
        v - h + 1 if wide(a) else v for a, v, h in zip(("gx", "gy", "gz"), (x, y, z), here)
    ]
    row_ids = (slot(found) * slots + at).astype(f32)
    ids = jnp.concatenate(
        [
            jnp.broadcast_to(row_ids[:, b * slots : (b + 1) * slots], (slots, slots)).T
            for b in range(blocks)
        ],
        axis=0,
    ).astype(jnp.int32)
    lanes = lax.broadcasted_iota(jnp.int32, (senders, slots), 1)
    count = table.shape[0]
    chosen = jnp.concatenate(
        [jnp.where(ids - k * slots == lanes, 1.0, 0.0).astype(bf16) for k in range(count)], axis=1
    )

    rel = w_rel[0].astype(f32)
    place_cols = jnp.transpose(jnp.broadcast_to(place[:1], (slots, slots)))
    recv = jnp.dot(latent, w_recv[0], preferred_element_type=f32) + b_first[...]
    for c in range(3):
        if c:
            place_cols = jnp.transpose(jnp.broadcast_to(place[c : c + 1], (slots, slots)))
        recv = recv - place_cols * rel[c : c + 1]
    recv_half[...] = 0.5 * recv

    for (when, _, arrival, _), (relay, _, _) in zip(sends, relays):

        def pass_on(arrival=arrival, relay=relay):
            arrival.wait_recv()
            if has_mate:
                relay.start()

        guarded(when, pass_on)
    if has_mate:
        mate_in.wait_recv()
        for (when, _, _, _), (_, mate_arrival, _) in zip(sends, relays):
            guarded(when, mate_arrival.wait_recv)

    gathered = jnp.dot(
        chosen, table[:, :slots, :].reshape(count * slots, width), preferred_element_type=f32
    ).astype(bf16)
    feats = jnp.zeros((senders, PACK), f32)
    for k in range(count):
        feats = feats + lax.dot_general(
            chosen[:, k * slots : (k + 1) * slots],
            table[k, slots:, :],
            (((1,), (1,)), ((), ())),
            preferred_element_type=f32,
        )
    send = jnp.dot(gathered, w_send[0], preferred_element_type=f32)
    square = jnp.zeros((senders, slots), f32)
    for c in range(3):
        where = feats[:, c : c + 1] + (feats[:, 3 + c : 4 + c] - here[c].astype(f32))
        where = jnp.broadcast_to(where, (senders, slots))
        send = send + where * rel[c : c + 1]
        apart = where - place[c : c + 1]
        square = square + apart * apart
    send_half[...] = (0.5 * send).astype(bf16)
    square = 0.25 * square
    scaled[...] = jnp.transpose(square)

    rel_half = (0.5 * rel[3:4]).astype(bf16)
    edge_half = 0.5 * w_edge[0].astype(f32)
    nil = jnp.zeros_like(edge_half)
    pair_edge[...] = jnp.concatenate(
        [jnp.concatenate([edge_half, nil], axis=1), jnp.concatenate([nil, edge_half], axis=1)], axis=0
    ).astype(bf16)
    alive = lax.broadcasted_iota(jnp.int32, (senders, width), 0) < counts_ref[0]
    masked[...] = jnp.where(alive, 0.5 * b_edge[...], -1e30).astype(bf16)

    @pl.loop(0, slots // GROUP)
    def _(group):
        base = pl.multiple_of(group * GROUP, GROUP)
        own_rows = recv_half[pl.ds(base, GROUP), :].astype(bf16)
        near = scaled[pl.ds(base, GROUP), :].astype(bf16)
        sums = []
        for i in range(0, GROUP, 2 * PAIRS):
            edges = []
            for p in range(PAIRS):
                halves = []
                for n in (i + 2 * p, i + 2 * p + 1):
                    s = jnp.concatenate(
                        [
                            jnp.transpose(jnp.broadcast_to(near[n : n + 1, b : b + slots], (width, slots)))
                            for b in range(0, senders, slots)
                        ],
                        axis=0,
                    )
                    pre = (own_rows[n : n + 1] + send_half[...]) + s * rel_half
                    halves.append(pre * (jnp.tanh(pre) + 1))
                edges.append(jnp.concatenate(halves, axis=1))
            msgs = jnp.dot(
                jnp.concatenate(edges, axis=0), pair_edge[...], preferred_element_type=f32
            ).astype(bf16)
            for n in range(2 * PAIRS):
                p, h = divmod(n, 2)
                msg = msgs[p * senders : (p + 1) * senders, h * width : (h + 1) * width]
                msg = msg + masked[...]
                msg = msg * (jnp.tanh(msg) + 1)
                total = jnp.zeros((8, width), f32)
                for b in range(0, senders, slots):
                    parts = [msg[r : r + PACK] for r in range(b, b + slots, PACK)]
                    while len(parts) > 1:
                        parts = [v + w for v, w in zip(parts[::2], parts[1::2])]
                    part = parts[0].astype(f32)
                    total = total + (part[:8] + part[8:])
                sums.append(jnp.sum(total, axis=0, keepdims=True))
        pooled[pl.ds(base, GROUP), :] = jnp.concatenate(sums, axis=0)

    mean = (pooled[...] / slots).astype(bf16)
    hidden = jax.nn.silu(
        jnp.dot(latent, w_self[0], preferred_element_type=f32)
        + jnp.dot(mean, w_agg[0], preferred_element_type=f32)
    ).astype(bf16)
    result = jnp.dot(hidden, w_out[0], preferred_element_type=f32)
    center = jnp.mean(result, axis=-1, keepdims=True)
    shifted = result - center
    spread = jnp.mean(shifted * shifted, axis=-1, keepdims=True)
    normed = shifted * lax.rsqrt(spread + 1e-05) * norm_gain[...]
    out_ref[0, 0, 0] = (latent.astype(f32) + normed).astype(bf16)

    for (when, copy, _, _), (relay, _, _) in zip(sends, relays):

        def finish(copy=copy, relay=relay):
            copy.wait_send()
            if has_mate:
                relay.wait_send()

        guarded(when, finish)
    if has_mate:
        mate_copy.wait_send()


def shards(latents, offsets, neighbours, counts, *weights):
    slots, width = latents.shape[3:]
    senders = neighbours.shape[3]
    count = slots_of("gx") * slots_of("gy") * slots_of("gz")
    routes = 9
    f32, bf16 = jnp.float32, jnp.bfloat16
    vmem = pl.BlockSpec(memory_space=pltpu.VMEM)
    args = (counts, latents, offsets, neighbours) + weights
    return pl.pallas_call(
        kernel,
        out_shape=jax.ShapeDtypeStruct(latents.shape, latents.dtype),
        in_specs=[pl.BlockSpec(memory_space=pl.ANY)] * INPUTS,
        out_specs=vmem,
        scratch_shapes=[pltpu.VMEM(a.shape, a.dtype) for a in args]
        + [
            pltpu.SemaphoreType.DMA((INPUTS,)),
            pltpu.VMEM((count, slots + PACK, width), bf16),
            pltpu.VMEM((slots, width), f32),
            pltpu.VMEM((senders, width), bf16),
            pltpu.VMEM((slots, senders), f32),
            pltpu.VMEM((slots, width), f32),
            pltpu.VMEM((2 * width, 2 * width), bf16),
            pltpu.VMEM((senders, width), bf16),
            pltpu.SemaphoreType.DMA((routes,)),
            pltpu.SemaphoreType.DMA((count,)),
            pltpu.SemaphoreType.DMA((routes,)),
        ],
        compiler_params=pltpu.CompilerParams(collective_id=0, has_side_effects=True),
    )(*args)


def solution(mesh):
    cells = ("groups", "gx"), "gy", "gz"
    in_specs = (P(*cells, None, None), P(*cells, None, None), P(*cells, None), P(*cells))
    in_specs += (P(),) * 10
    return jax.shard_map(
        shards, mesh=mesh, in_specs=in_specs, out_specs=P(*cells, None, None), check_vma=False
    )
```

```python
import functools

import jax
import jax.numpy as jnp
from jax import lax
from jax.experimental import pallas as pl
from jax.experimental.pallas import tpu as pltpu
from jax.sharding import PartitionSpec as P

MESH = pl.DeviceIdType.MESH
PACK = 16
GROUP = 32
PAIRS = 1
INPUTS = 14
LOAD_ORDER = (1, 2, 3, 0) + tuple(range(4, 14))


def split(value, size):
    if size & (size - 1) == 0:
        return value >> (size.bit_length() - 1), value & (size - 1)
    return lax.div(value, size), lax.rem(value, size)


def wide(axis):
    return lax.axis_size(axis) > 2


def slots_of(axis):
    return min(lax.axis_size(axis), 3)


def moves(axis):
    size, here = lax.axis_size(axis), lax.axis_index(axis)
    if size == 1:
        return []
    if size == 2:
        return [(1 - here, None)]
    return [(here - 1, here > 0), (here + 1, here < size - 1)]


def slot_on(axis, source, target):
    return source - target + 1 if wide(axis) else source


def both(a, b):
    if a is None:
        return b
    return a if b is None else jnp.logical_and(a, b)


def guarded(condition, action):
    if condition is None:
        action()
    else:
        pl.when(condition)(action)


def kernel(*refs):
    hbm, out_ref, held, scratch = refs[:INPUTS], refs[INPUTS], refs[INPUTS + 1 : 2 * INPUTS + 1], refs[2 * INPUTS + 1 :]
    load_sem, table, recv_half, send_half, scaled, pooled, pair_edge, masked, chosen = scratch[:9]
    send_sem, recv_sem, relay_sem = scratch[9:]
    (
        counts_ref, latents_ref, offsets_ref, neighbours_ref, w_recv, w_send, w_rel, b_first,
        w_edge, b_edge, w_self, w_agg, w_out, norm_gain,
    ) = held
    loads = [
        pltpu.make_async_copy(src, dst, load_sem.at[n]) for n, (src, dst) in enumerate(zip(hbm, held))
    ]
    for n in LOAD_ORDER:
        loads[n].start()
    f32, bf16 = jnp.float32, jnp.bfloat16
    slots, width = latents_ref.shape[3], latents_ref.shape[4]
    senders = neighbours_ref.shape[3]
    blocks = senders // slots
    here = [lax.axis_index(axis) for axis in ("gx", "gy", "gz")]
    sizes = [lax.axis_size(axis) for axis in ("gx", "gy", "gz")]
    spans = [slots_of(axis) for axis in ("gx", "gy", "gz")]

    def slot(coords):
        return (coords[0] * spans[1] + coords[1]) * spans[2] + coords[2]

    own_coords = [slot_on(a, c, c) for a, c in zip(("gx", "gy", "gz"), here)]
    own = slot(own_coords)

    stay_x, stay_y = (here[0], None), (here[1], None)
    routes = []
    for x, when_x in [stay_x] + moves("gx"):
        for y, when_y in [stay_y] + moves("gy"):
            if x is here[0] and y is here[1]:
                continue
            routes.append((x, y, both(when_x, when_y)))
    routes.sort(key=lambda r: (r[0] is not here[0]) + (r[1] is not here[1]))
    has_mate = sizes[2] > 1
    mate = {"gz": 1 - here[2]}

    barrier = pltpu.get_barrier_semaphore()

    def hello(target):
        pl.semaphore_signal(barrier, inc=1, device_id=target, device_id_type=MESH)

    if has_mate:
        hello(mate)
    for x, y, when in routes:
        guarded(when, functools.partial(hello, {"gx": x, "gy": y}))
    for n in (1, 2):
        loads[n].wait()
    latent = latents_ref[0, 0, 0]
    place = offsets_ref[0, 0, 0].astype(f32)
    rows = lax.broadcasted_iota(jnp.int32, (PACK, slots), 0)
    extra = jnp.zeros((PACK, slots), f32)
    for c in range(3):
        extra = jnp.where(rows == c, place[c : c + 1, :], extra)
        extra = jnp.where(rows == 3 + c, here[c].astype(f32), extra)
    table[own, :slots, :] = latent
    table[own, slots:, :] = extra.astype(bf16)

    peers = jnp.int32(1 if has_mate else 0)
    for x, y, when in routes:
        peers = peers + (1 if when is None else when.astype(jnp.int32))
    pl.semaphore_wait(barrier, peers)

    sends, relays = [], []
    for n, (x, y, when) in enumerate(routes):
        there = slot(
            [slot_on("gx", here[0], x), slot_on("gy", here[1], y), slot_on("gz", here[2], here[2])]
        )
        mine = slot(
            [slot_on("gx", x, here[0]), slot_on("gy", y, here[1]), slot_on("gz", here[2], here[2])]
        )
        copy = pltpu.make_async_remote_copy(
            src_ref=table.at[own],
            dst_ref=table.at[there],
            send_sem=send_sem.at[n],
            recv_sem=recv_sem.at[there],
            device_id={"gx": x, "gy": y},
            device_id_type=MESH,
        )
        arrival = pltpu.make_async_remote_copy(
            src_ref=table.at[own],
            dst_ref=table.at[mine],
            send_sem=send_sem.at[n],
            recv_sem=recv_sem.at[mine],
            device_id={"gx": x, "gy": y},
            device_id_type=MESH,
        )
        relay = pltpu.make_async_remote_copy(
            src_ref=table.at[mine],
            dst_ref=table.at[mine],
            send_sem=relay_sem.at[n],
            recv_sem=recv_sem.at[mine],
            device_id=mate,
            device_id_type=MESH,
        )
        mate_slot = slot(
            [slot_on("gx", x, here[0]), slot_on("gy", y, here[1]), 1 - here[2]]
        )
        mate_arrival = pltpu.make_async_remote_copy(
            src_ref=table.at[own],
            dst_ref=table.at[mate_slot],
            send_sem=relay_sem.at[n],
            recv_sem=recv_sem.at[mate_slot],
            device_id=mate,
            device_id_type=MESH,
        )
        sends.append((when, copy, arrival, mine))
        relays.append((relay, mate_arrival, mate_slot))
    last = len(routes)
    if has_mate:
        mate_own = slot([own_coords[0], own_coords[1], 1 - here[2]])
        mate_copy = pltpu.make_async_remote_copy(
            src_ref=table.at[own], dst_ref=table.at[own], send_sem=send_sem.at[last],
            recv_sem=recv_sem.at[own], device_id=mate, device_id_type=MESH,
        )
        mate_in = pltpu.make_async_remote_copy(
            src_ref=table.at[own], dst_ref=table.at[mate_own], send_sem=send_sem.at[last],
            recv_sem=recv_sem.at[mate_own], device_id=mate, device_id_type=MESH,
        )
    for when, copy, _, _ in sends:
        guarded(when, copy.start)
    if has_mate:
        mate_copy.start()

    def clear(which):
        table[which] = jnp.zeros(table.shape[1:], bf16)

    for (when, _, _, mine), (_, _, mate_slot) in zip(sends, relays):
        if when is not None:
            pl.when(jnp.logical_not(when))(functools.partial(clear, mine))
            if has_mate:
                pl.when(jnp.logical_not(when))(functools.partial(clear, mate_slot))

    loads[0].wait()
    for n in range(3, INPUTS):
        loads[n].wait()
    cell, at = split(neighbours_ref[0, 0], slots)
    cell, z = split(cell, sizes[2])
    x, y = split(cell, sizes[1])
    found = [
        v - h + 1 if wide(a) else v for a, v, h in zip(("gx", "gy", "gz"), (x, y, z), here)
    ]
    row_ids = (slot(found) * slots + at).astype(f32)
    ids = jnp.concatenate(
        [
            jnp.broadcast_to(row_ids[:, b * slots : (b + 1) * slots], (slots, slots)).T
            for b in range(blocks)
        ],
        axis=0,
    ).astype(jnp.int32)
    lanes = lax.broadcasted_iota(jnp.int32, (senders, slots), 1)
    count = table.shape[0]
    span_z = spans[2]
    for k in range(count):
        chosen[k // span_z, :, (k % span_z) * slots : (k % span_z + 1) * slots] = jnp.where(
            ids - k * slots == lanes, 1.0, 0.0
        ).astype(bf16)

    rel = w_rel[0].astype(f32)
    place_cols = jnp.transpose(jnp.broadcast_to(place[:1], (slots, slots)))
    recv = jnp.dot(latent, w_recv[0], preferred_element_type=f32) + b_first[...]
    for c in range(3):
        if c:
            place_cols = jnp.transpose(jnp.broadcast_to(place[c : c + 1], (slots, slots)))
        recv = recv - place_cols * rel[c : c + 1]
    recv_half[...] = 0.5 * recv

    def gather(line, carry):
        picks, cells = chosen[line], table.at[pl.ds(line * span_z, span_z)]
        found = jnp.dot(
            picks, cells[:, :slots, :].reshape(span_z * slots, width), preferred_element_type=f32
        )
        marks = cells[:, slots:, :]
        marks = jnp.concatenate([marks[k] for k in range(span_z)], axis=1)
        feats = lax.dot_general(picks, marks, (((1,), (1,)), ((), ())), preferred_element_type=f32)
        return (found, feats) if carry is None else (carry[0] + found, carry[1] + feats)

    if has_mate:
        mate_in.wait_recv()
    carry = gather(slot([own_coords[0], own_coords[1], 0]) // span_z, None)
    for (when, _, arrival, _), (relay, _, _) in zip(sends, relays):

        def pass_on(arrival=arrival, relay=relay):
            arrival.wait_recv()
            if has_mate:
                relay.start()

        guarded(when, pass_on)
    for (when, _, _, mine), (_, mate_arrival, _) in zip(sends, relays):
        if has_mate:
            guarded(when, mate_arrival.wait_recv)
        carry = gather(mine // span_z, carry)
    gathered, feats = carry[0].astype(bf16), carry[1]
    send = jnp.dot(gathered, w_send[0], preferred_element_type=f32)
    square = jnp.zeros((senders, slots), f32)
    for c in range(3):
        where = feats[:, c : c + 1] + (feats[:, 3 + c : 4 + c] - here[c].astype(f32))
        where = jnp.broadcast_to(where, (senders, slots))
        send = send + where * rel[c : c + 1]
        apart = where - place[c : c + 1]
        square = square + apart * apart
    send_half[...] = (0.5 * send).astype(bf16)
    square = 0.25 * square
    scaled[...] = jnp.transpose(square)

    rel_half = (0.5 * rel[3:4]).astype(bf16)
    edge_half = 0.5 * w_edge[0].astype(f32)
    nil = jnp.zeros_like(edge_half)
    pair_edge[...] = jnp.concatenate(
        [jnp.concatenate([edge_half, nil], axis=1), jnp.concatenate([nil, edge_half], axis=1)], axis=0
    ).astype(bf16)
    alive = lax.broadcasted_iota(jnp.int32, (senders, width), 0) < counts_ref[0]
    masked[...] = jnp.where(alive, 0.5 * b_edge[...], -1e30).astype(bf16)

    @pl.loop(0, slots // GROUP)
    def _(group):
        base = pl.multiple_of(group * GROUP, GROUP)
        own_rows = recv_half[pl.ds(base, GROUP), :].astype(bf16)
        near = scaled[pl.ds(base, GROUP), :].astype(bf16)
        sums = []
        for i in range(0, GROUP, 2 * PAIRS):
            edges = []
            for p in range(PAIRS):
                halves = []
                for n in (i + 2 * p, i + 2 * p + 1):
                    s = jnp.concatenate(
                        [
                            jnp.transpose(jnp.broadcast_to(near[n : n + 1, b : b + slots], (width, slots)))
                            for b in range(0, senders, slots)
                        ],
                        axis=0,
                    )
                    pre = (own_rows[n : n + 1] + send_half[...]) + s * rel_half
                    halves.append(pre * (jnp.tanh(pre) + 1))
                edges.append(jnp.concatenate(halves, axis=1))
            msgs = jnp.dot(
                jnp.concatenate(edges, axis=0), pair_edge[...], preferred_element_type=f32
            ).astype(bf16)
            for n in range(2 * PAIRS):
                p, h = divmod(n, 2)
                msg = msgs[p * senders : (p + 1) * senders, h * width : (h + 1) * width]
                msg = msg + masked[...]
                msg = msg * (jnp.tanh(msg) + 1)
                total = jnp.zeros((8, width), f32)
                for b in range(0, senders, slots):
                    parts = [msg[r : r + PACK] for r in range(b, b + slots, PACK)]
                    while len(parts) > 1:
                        parts = [v + w for v, w in zip(parts[::2], parts[1::2])]
                    part = parts[0].astype(f32)
                    total = total + (part[:8] + part[8:])
                sums.append(jnp.sum(total, axis=0, keepdims=True))
        pooled[pl.ds(base, GROUP), :] = jnp.concatenate(sums, axis=0)

    mean = (pooled[...] / slots).astype(bf16)
    hidden = jax.nn.silu(
        jnp.dot(latent, w_self[0], preferred_element_type=f32)
        + jnp.dot(mean, w_agg[0], preferred_element_type=f32)
    ).astype(bf16)
    result = jnp.dot(hidden, w_out[0], preferred_element_type=f32)
    center = jnp.mean(result, axis=-1, keepdims=True)
    shifted = result - center
    spread = jnp.mean(shifted * shifted, axis=-1, keepdims=True)
    normed = shifted * lax.rsqrt(spread + 1e-05) * norm_gain[...]
    out_ref[0, 0, 0] = (latent.astype(f32) + normed).astype(bf16)

    for (when, copy, _, _), (relay, _, _) in zip(sends, relays):

        def finish(copy=copy, relay=relay):
            copy.wait_send()
            if has_mate:
                relay.wait_send()

        guarded(when, finish)
    if has_mate:
        mate_copy.wait_send()


def shards(latents, offsets, neighbours, counts, *weights):
    slots, width = latents.shape[3:]
    senders = neighbours.shape[3]
    count = slots_of("gx") * slots_of("gy") * slots_of("gz")
    routes = 9
    f32, bf16 = jnp.float32, jnp.bfloat16
    vmem = pl.BlockSpec(memory_space=pltpu.VMEM)
    args = (counts, latents, offsets, neighbours) + weights
    return pl.pallas_call(
        kernel,
        out_shape=jax.ShapeDtypeStruct(latents.shape, latents.dtype),
        in_specs=[pl.BlockSpec(memory_space=pl.ANY)] * INPUTS,
        out_specs=vmem,
        scratch_shapes=[pltpu.VMEM(a.shape, a.dtype) for a in args]
        + [
            pltpu.SemaphoreType.DMA((INPUTS,)),
            pltpu.VMEM((count, slots + PACK, width), bf16),
            pltpu.VMEM((slots, width), f32),
            pltpu.VMEM((senders, width), bf16),
            pltpu.VMEM((slots, senders), f32),
            pltpu.VMEM((slots, width), f32),
            pltpu.VMEM((2 * width, 2 * width), bf16),
            pltpu.VMEM((senders, width), bf16),
            pltpu.VMEM((count // slots_of("gz"), senders, slots * slots_of("gz")), bf16),
            pltpu.SemaphoreType.DMA((routes,)),
            pltpu.SemaphoreType.DMA((count,)),
            pltpu.SemaphoreType.DMA((routes,)),
        ],
        compiler_params=pltpu.CompilerParams(collective_id=0, has_side_effects=True),
    )(*args)


def solution(mesh):
    cells = ("groups", "gx"), "gy", "gz"
    in_specs = (P(*cells, None, None), P(*cells, None, None), P(*cells, None), P(*cells))
    in_specs += (P(),) * 10
    return jax.shard_map(
        shards, mesh=mesh, in_specs=in_specs, out_specs=P(*cells, None, None), check_vma=False
    )
```
